32 devices in a mesh: section: 2 (over core), seq: 4 (over y, x), mp: 4 (over z).
Axes of the slice: x: 2, y: 2, z: 4, core: 2. Of those that a mesh axis runs over, the one named last changes fastest.
Arguments:
- token_ids: int32 [2, 1024], P(None, 'seq'), may hold values from 0 to 511
- embed_table: bfloat16 [512, 4096], P(None, 'mp'), may hold values from -40 to 40
- norm_gain: bfloat16 [2, 4096], P('section', 'mp'), may hold values from 0.099609375 to 1.8984375
- short_filters: bfloat16 [2, 3, 7, 4096], P('section', None, None, 'mp'), may hold values from -2 to 2
- medium_filters: bfloat16 [2, 128, 4096], P('section', None, 'mp'), may hold values from -0.5 to 0.5
- out_weight: bfloat16 [2, 4096, 4096], P('section', 'seq', 'mp'), may hold values from -0.09375 to 0.09375
Outputs:
- streams: bfloat16 [2, 2, 1024, 4096], P('section', None, 'seq', 'mp')
The draws below stay inside these ranges and needn't reach their ends.
All inputs are finite; a program needn't handle non-finite values.
Results may differ from the reference program's by a relative error of at most 0.018.
Values may be sent and summed in bfloat16 or wider, within the bound.
A program may use at most 64 MiB of HBM per device.

```python
import math
import jax
import jax.numpy as jnp
import numpy as np
from jax import lax

D = 4096
VOCAB = 512
SHORT_LEN = 7
MR_LEN = 128
MICRO = 2
SEQ_LEN = 1024
N_SECTION = 2


def draw_embed_table(key, part):
    base_key, row_key, col_key = jax.random.split(key, 3)
    base = jnp.clip(jax.random.normal(base_key, (VOCAB, D), jnp.float32), -4.0, 4.0)
    row_scale = jnp.exp(jax.random.uniform(row_key, (VOCAB, 1), jnp.float32, math.log(0.5), math.log(2.0)))
    col_scale = jnp.exp(jax.random.uniform(col_key, (1, D), jnp.float32, math.log(0.5), math.log(2.5)))
    ramp = 0.6 * jnp.exp(math.log(3.0) * jnp.arange(D, dtype=jnp.float32)[None, :] / D)
    return (base * row_scale * col_scale * ramp).astype(jnp.bfloat16)


def with_ends(array, own_key, least, high):
    longest = array.shape.index(max(array.shape))
    spots = []
    for shift in (0, 1):
        where = [jax.random.randint(jax.random.fold_in(own_key, axis), (), 0, length) for axis, length in enumerate(array.shape)]
        where[longest] = (where[longest] + shift) % array.shape[longest]
        spots.append(tuple(where))
    return array.at[spots[0]].set(least).at[spots[1]].set(high)


def level_of(stream_key, dims, shards, smallest, high):
    def one(position, parts):
        draws = jax.random.uniform(jax.random.fold_in(jax.random.fold_in(stream_key, 6), position), (parts,), jnp.float32, smallest / len(shards), high / len(shards))
        return jnp.repeat(jnp.exp(draws), dims[position] // parts).reshape((-1,) + (1,) * (len(dims) - position - 1))

    level = one(*shards[0])
    for cut in shards[1:]:
        level = level * one(*cut)
    return level


def cumulative_ranks(number_of, slope):
    weights = [(1 << 20) // math.isqrt(standing ** slope) + 1 for standing in range(1, number_of + 1)]
    deviation = 1 + sum(weights) // (1 << 30)
    return np.cumsum(np.array([max(1, weight // deviation) for weight in weights]))


def ranked(own_key, shape, count, slope):
    grid = cumulative_ranks(count, slope)
    lot = jax.random.randint(jax.random.fold_in(own_key, 1), shape, 0, int(grid[count - 1]))
    grade = jnp.searchsorted(jnp.asarray(grid, jnp.int32), lot, side="right")
    return jax.random.permutation(jax.random.fold_in(own_key, 2), count)[grade].astype(jnp.int32)


def centred(own_key, dims, scale, bound, cuts=(), held_as=jnp.bfloat16):
    loudness = level_of(own_key, dims, cuts, -0.22, 0.18) if cuts else 1.0
    array = jax.random.normal(own_key, dims, jnp.float32) * scale * loudness
    return jnp.minimum(jnp.maximum(array, -bound), bound).astype(held_as)


def setup_inputs(seed: int = 0) -> dict:
    keys = jax.random.split(jax.random.key(seed), 7)
    return {
        "token_ids": with_ends(ranked(keys[0], (MICRO, SEQ_LEN), VOCAB, 2), jax.random.fold_in(keys[0], 3), 0, VOCAB - 1).astype(jnp.int32),
        "embed_table": draw_embed_table(jax.random.fold_in(keys[6], 71), 0),
        "norm_gain": jnp.clip(1.0 + 0.18 * jax.random.normal(keys[2], (N_SECTION, D), jnp.float32), 0.099609375, 1.8984375).astype(jnp.bfloat16),
        "short_filters": centred(keys[3], (N_SECTION, 3, SHORT_LEN, D), SHORT_LEN ** -0.5, 2.0, ((0, 2), (3, 4))),
        "medium_filters": centred(keys[4], (N_SECTION, MR_LEN, D), MR_LEN ** -0.5, 0.5, ((0, 2), (2, 4))),
        "out_weight": centred(keys[5], (N_SECTION, D, D), D ** -0.5, 0.09375, ((0, 2), (1, 4), (2, 4))),
    }


def causal_filter(signal, taps):
    length = taps.shape[0]
    total_rows = signal.shape[0]
    padded = jnp.pad(signal.astype(jnp.float32), ((length - 1, 0), (0, 0)))
    taps_wide = taps.astype(jnp.float32)

    def add_tap(index, total):
        start = (length - 1 - index).astype(jnp.int32)
        window = lax.dynamic_slice_in_dim(padded, start, total_rows, 0)
        return total + taps_wide[index][None, :] * window
    initial = jnp.zeros((total_rows, signal.shape[1]), jnp.float32)
    return lax.fori_loop(jnp.int32(0), jnp.int32(length), add_tap, initial)

def mixer_layer(stream_in, gain, shorts, medium, weight):
    stream = stream_in.astype(jnp.float32)
    mean_square = lax.optimization_barrier(jnp.sum(stream * stream, axis=1, keepdims=True)) / D
    normed = (stream * lax.rsqrt(mean_square + 1e-06) * gain.astype(jnp.float32)[None, :]).astype(jnp.bfloat16)
    features = [causal_filter(normed, shorts[index]).astype(jnp.bfloat16) for index in range(3)]
    product = (features[1].astype(jnp.float32) * features[2].astype(jnp.float32)).astype(jnp.bfloat16)
    filtered = causal_filter(product, medium)
    gated = (features[0].astype(jnp.float32) * filtered).astype(jnp.bfloat16)
    projected = jnp.dot(gated, weight, preferred_element_type=jnp.float32)
    return (stream + projected).astype(jnp.bfloat16)

def reference(token_ids, embed_table, norm_gain, short_filters, medium_filters, out_weight):
    results = []
    for micro_index in range(MICRO):
        stream = embed_table[token_ids[micro_index]]
        per_section = []
        for section_index in range(N_SECTION):
            stream = mixer_layer(stream, norm_gain[section_index], short_filters[section_index], medium_filters[section_index], out_weight[section_index])
            per_section.append(stream)
        results.append(jnp.stack(per_section))
    return jnp.stack(results, axis=1)
```

```python
import functools

import jax
import jax.numpy as jnp
from jax import lax
from jax.experimental import pallas as pl
from jax.experimental.pallas import tpu as pltpu
from jax.sharding import PartitionSpec as P

MESH = pl.DeviceIdType.MESH
LANES = 128
BF = jnp.bfloat16
F32 = jnp.float32


def relay_kernel(
    sizes,
    emb_ref, gain_ref, short_ref, med_ref, w_ref,
    out_ref,
    wbuf, inbuf, x, colb, sqbuf, nsend, nrim, nf, qf, ext, psend, prim, sh, medf, gbuf, acc,
    own_sem, w_send, w_recv, go_sem, in_send, in_recv, sq_send, sq_recv,
    n_send, n_recv, p_send, p_recv, up_send, up_recv, dn_send, dn_recv,
):
    n_sec, n_seq, n_mp = sizes
    micro, rows, width = emb_ref.shape
    total_width = width * n_mp
    short_len = short_ref.shape[0] // 3
    med_len = med_ref.shape[0]
    rim = psend.shape[1]
    nrim_rows = nsend.shape[1]
    blocks = rows // rim
    depth = w_ref.shape[0]
    half = depth // 2
    levels = n_seq.bit_length() - 1
    sec, seq, mp = lax.axis_index("section"), lax.axis_index("seq"), lax.axis_index("mp")

    def remote(src, dst, send, recv, **where):
        return pltpu.make_async_remote_copy(
            src_ref=src, dst_ref=dst, send_sem=send, recv_sem=recv,
            device_id=where, device_id_type=MESH,
        )

    own = pltpu.make_async_copy(
        w_ref, wbuf.at[pl.ds(pl.multiple_of(seq * depth, depth), depth)], own_sem
    )
    own.start()
    barrier = pltpu.get_barrier_semaphore()
    greeted = 0
    for axis, count, index in (("section", n_sec, sec), ("seq", n_seq, seq), ("mp", n_mp, mp)):
        for step in range(1, count):
            pl.semaphore_signal(
                barrier, inc=1, device_id={axis: lax.rem(index + step, count)}, device_id_type=MESH
            )
            greeted += 1
    pl.semaphore_wait(barrier, greeted)
    own.wait()

    def bit_of(bit):
        return lax.rem(lax.div(seq, jnp.int32(1 << bit)), jnp.int32(2))

    orders = (list(range(levels)), list(reversed(range(levels))))

    def weight_copies(level, incoming=False):
        made = []
        for part in range(2):
            order = orders[part]
            flip = order[level]
            partner = seq + (1 - 2 * bit_of(flip)) * (1 << flip)
            for k in range(1 << level):
                shard = seq
                theirs = partner
                for i in range(level):
                    change = (((k >> i) & 1) - bit_of(order[i])) * (1 << order[i])
                    shard = shard + change
                    theirs = theirs + change
                slot = (1 << level) - 1 + k
                start = pl.multiple_of((theirs if incoming else shard) * depth + part * half, half)
                place = wbuf.at[pl.ds(start, half)]
                made.append(remote(place, place, w_send.at[part, slot], w_recv.at[part, slot], seq=partner))
        return made

    def weights_start(level):
        for out in weight_copies(level):
            out.start()

    def weights_arrive(level):
        for into in weight_copies(level, True):
            into.wait_recv()

    def weights_forward():
        for level in range(1, levels):
            weights_arrive(level - 1)
            weights_start(level)

    @pl.when(sec > 0)
    def _():
        pl.semaphore_wait(go_sem, 1)

    weights_start(0)

    @pl.when(sec > 0)
    def _():
        weights_forward()

    medf[...] = med_ref[...].astype(F32)

    @pl.when(seq == 0)
    def _():
        nf[0:nrim_rows, :] = jnp.zeros((nrim_rows, width), F32)
        ext[0:rim, :] = jnp.zeros((rim, width), F32)

    def lane(c):
        return pl.ds(pl.multiple_of(c * LANES, LANES), LANES)

    chunks = width // LANES

    def relay_copy(m):
        return remote(out_ref.at[m], inbuf.at[m], in_send.at[m], in_recv.at[m], section=sec + 1)

    def relay_in(m):
        return remote(inbuf.at[m], inbuf.at[m], in_send.at[m], in_recv.at[m], section=sec)

    def square_copy(m, step):
        return remote(
            sqbuf.at[m, mp], sqbuf.at[m, mp], sq_send.at[m, step - 1], sq_recv.at[m, step - 1],
            mp=lax.rem(mp + step, n_mp),
        )

    def square_in(m, step):
        place = sqbuf.at[m, lax.rem(mp + n_mp - step, n_mp)]
        return remote(
            place, place, sq_send.at[m, step - 1], sq_recv.at[m, step - 1],
            mp=lax.rem(mp + step, n_mp),
        )

    def normed_copy(m):
        return remote(nsend.at[m], nrim.at[m], n_send.at[m], n_recv.at[m], seq=seq + 1)

    def product_copy(m):
        return remote(psend.at[m], prim.at[m], p_send.at[m], p_recv.at[m], seq=seq + 1)

    def line_copy(m, block, step, piece, up):
        place = gbuf.at[m, block, pl.ds(piece * rim, rim)]
        send, recv = (up_send, up_recv) if up else (dn_send, dn_recv)
        return remote(
            place, place, send.at[m, step, piece], recv.at[m, step, piece],
            mp=(mp + 1) if up else (mp - 1),
        )

    def gated_send(m, block, step, piece, up):
        room = (mp < n_mp - 1) if up else (mp > 0)

        @pl.when(room)
        def _():
            line_copy(m, block, step, piece, up).start()

    row_chunk = 32

    for m in range(micro):
        @pl.when(sec > 0)
        def _():
            relay_in(m).wait_recv()

        def squares(i, _):
            part = pl.ds(pl.multiple_of(i * row_chunk, row_chunk), row_chunk)

            @pl.when(sec == 0)
            def _():
                x[part, :] = emb_ref[m, part, :].astype(F32)

            @pl.when(sec > 0)
            def _():
                x[part, :] = inbuf[m, part, :].astype(F32)

            value = x[part, :]
            summed = jnp.sum(value * value, axis=1, keepdims=True)
            colb[part, :] = jnp.broadcast_to(summed, (row_chunk, LANES))
            return 0

        lax.fori_loop(0, rows // row_chunk, squares, 0)
        sqbuf[m, mp] = colb[...].T[0:8]
        for step in range(1, n_mp):
            square_copy(m, step).start()
        for step in range(1, n_mp):
            square_in(m, step).wait_recv()
        total = sqbuf[m, 0]
        for j in range(1, n_mp):
            total = total + sqbuf[m, j]
        scale = lax.rsqrt(total / total_width + 1e-06)
        colb[...] = jnp.broadcast_to(scale[0:1], (LANES, rows)).T

        def normalise(c, _):
            value = x[:, lane(c)] * colb[...] * gain_ref[0:1, lane(c)]
            rounded = value.astype(BF)
            nf[pl.ds(nrim_rows, rows), lane(c)] = rounded.astype(F32)
            nsend[m, :, lane(c)] = rounded[rows - nrim_rows:]
            return 0

        lax.fori_loop(0, chunks, normalise, 0)

        @pl.when(seq < n_seq - 1)
        def _():
            normed_copy(m).start()

        def features(block):
            sub = rim // 2

            def body(c, _):
                for piece in range(2):
                    base = block * rim + piece * sub
                    made = [None, None, None]
                    for s in range(short_len):
                        window = nf[pl.ds(nrim_rows + base - s, sub), lane(c)]
                        for f in range(3):
                            term = short_ref[pl.ds(f * short_len + s, 1), lane(c)] * window
                            made[f] = term if made[f] is None else made[f] + term
                    made = [value.astype(BF).astype(F32) for value in made]
                    product = (made[1] * made[2]).astype(BF)
                    qf[pl.ds(base, sub), lane(c)] = made[0]
                    ext[pl.ds(rim + base, sub), lane(c)] = product.astype(F32)
                    if block == blocks - 1:
                        psend[m, pl.ds(piece * sub, sub), lane(c)] = product
                return 0

            lax.fori_loop(0, chunks, body, 0)

        for block in reversed(range(blocks)):
            if block == 0:
                @pl.when(seq > 0)
                def _():
                    normed_copy(m).wait_recv()
                    nf[0:nrim_rows, :] = nrim[m].astype(F32)

            features(block)
            if block == blocks - 1:
                @pl.when(seq < n_seq - 1)
                def _():
                    product_copy(m).start()

        if m == 0:
            @pl.when(sec == 0)
            def _():
                weights_forward()

        def filtering(block):
            taps_rows = 2 * rim

            def body(c, _):
                lo = block * rim
                for b in range(8):
                    sh[b, 8:taps_rows, :] = ext[pl.ds(lo + 8 - b, taps_rows - 8), lane(c)]
                value = jnp.zeros((rim, LANES), F32)
                for b in range(8):
                    for a in range(rim // 8):
                        s = 8 * a + b
                        if s < med_len:
                            tap = medf[pl.ds(s, 1), lane(c)]
                            value = value + tap * sh[b, rim - 8 * a:2 * rim - 8 * a, :]
                here = pl.ds(lo, rim)
                gbuf[m, mp, here, lane(c)] = (qf[here, lane(c)] * value).astype(BF)
                return 0

            lax.fori_loop(0, chunks, body, 0)

        for block in reversed(range(blocks)):
            if block == 0:
                @pl.when(seq > 0)
                def _():
                    product_copy(m).wait_recv()
                    ext[0:rim, :] = prim[m].astype(F32)

            filtering(block)
            for up in (True, False):
                gated_send(m, mp, 0, block, up)

        if m == 0:
            weights_arrive(levels - 1)

            @pl.when(sec < n_sec - 1)
            def _():
                pl.semaphore_signal(go_sem, inc=1, device_id={"section": sec + 1}, device_id_type=MESH)

        cols = 256

        def add_block(block, first):
            source = pl.ds(pl.multiple_of(block * width, width), width)

            def body(c, _):
                part = pl.ds(pl.multiple_of(c * cols, cols), cols)
                value = jnp.dot(gbuf[m, block], wbuf[source, part], preferred_element_type=F32)
                if first:
                    acc[:, part] = value
                else:
                    acc[:, part] += value
                return 0

            lax.fori_loop(0, width // cols, body, 0)

        add_block(mp, True)
        for step in range(1, n_mp):
            for up in (True, False):
                here = (mp - step) if up else (mp + step)
                exists = (here >= 0) if up else (here < n_mp)

                @pl.when(exists)
                def _():
                    for piece in reversed(range(blocks)):
                        line_copy(m, here, step - 1, piece, up).wait_recv()
                        if step < n_mp - 1:
                            gated_send(m, here, step, piece, up)
                    add_block(here, False)

        def finish(i, _):
            part = pl.ds(pl.multiple_of(i * row_chunk, row_chunk), row_chunk)
            out_ref[m, part, :] = (x[part, :] + acc[part, :]).astype(BF)
            return 0

        lax.fori_loop(0, rows // row_chunk, finish, 0)

        @pl.when(sec < n_sec - 1)
        def _():
            relay_copy(m).start()

    for level in range(levels):
        for out in weight_copies(level):
            out.wait_send()
    for m in range(micro):
        @pl.when(sec < n_sec - 1)
        def _():
            relay_copy(m).wait_send()

        for step in range(1, n_mp):
            square_copy(m, step).wait_send()

        @pl.when(seq < n_seq - 1)
        def _():
            normed_copy(m).wait_send()
            product_copy(m).wait_send()

        for up in (True, False):
            room = (mp < n_mp - 1) if up else (mp > 0)
            for step in range(n_mp - 1):
                block = (mp - step) if up else (mp + step)
                exists = (block >= 0) if up else (block < n_mp)

                @pl.when(jnp.logical_and(room, exists))
                def _():
                    for piece in range(blocks):
                        line_copy(m, block, step, piece, up).wait_send()


def up16(count):
    return (count + 15) // 16 * 16


def local(sizes, token_ids, embed_table, norm_gain, short_filters, medium_filters, out_weight):
    n_sec, n_seq, n_mp = sizes
    micro, rows = token_ids.shape
    vocab, width = embed_table.shape
    ids = token_ids.reshape(micro * rows)
    one_hot = (ids[:, None] == lax.broadcasted_iota(jnp.int32, (micro * rows, vocab), 1)).astype(BF)
    embedded = jnp.dot(one_hot, embed_table, preferred_element_type=F32).astype(BF)
    embedded = embedded.reshape(micro, rows, width)
    shorts = short_filters[0].astype(F32).reshape(-1, width)
    nrim_rows = up16(short_filters.shape[2] - 1)
    rim = up16(medium_filters.shape[1])
    blocks = rows // rim
    vmem = pl.BlockSpec(memory_space=pltpu.VMEM)
    dma = pltpu.SemaphoreType.DMA
    result = pl.pallas_call(
        functools.partial(relay_kernel, sizes),
        out_shape=jax.ShapeDtypeStruct((micro, rows, width), BF),
        in_specs=[vmem, vmem, vmem, vmem, pl.BlockSpec(memory_space=pl.ANY)],
        out_specs=vmem,
        scratch_shapes=[
            pltpu.VMEM((width * n_mp, width), BF),
            pltpu.VMEM((micro, rows, width), BF),
            pltpu.VMEM((rows, width), F32),
            pltpu.VMEM((rows, LANES), F32),
            pltpu.VMEM((micro, n_mp, 8, rows), F32),
            pltpu.VMEM((micro, nrim_rows, width), BF),
            pltpu.VMEM((micro, nrim_rows, width), BF),
            pltpu.VMEM((nrim_rows + rows, width), F32),
            pltpu.VMEM((rows, width), F32),
            pltpu.VMEM((rim + rows, width), F32),
            pltpu.VMEM((micro, rim, width), BF),
            pltpu.VMEM((micro, rim, width), BF),
            pltpu.VMEM((8, 2 * rim, LANES), F32),
            pltpu.VMEM(medium_filters.shape[1:], F32),
            pltpu.VMEM((micro, n_mp, rows, width), BF),
            pltpu.VMEM((rows, width), F32),
            dma, dma((2, n_seq)), dma((2, n_seq)), pltpu.SemaphoreType.REGULAR,
            dma((micro,)), dma((micro,)), dma((micro, n_mp)), dma((micro, n_mp)),
            dma((micro,)), dma((micro,)), dma((micro,)), dma((micro,)),
            dma((micro, n_mp, blocks)), dma((micro, n_mp, blocks)),
            dma((micro, n_mp, blocks)), dma((micro, n_mp, blocks)),
        ],
        compiler_params=pltpu.CompilerParams(
            collective_id=0, has_side_effects=True, vmem_limit_bytes=56 * 1024 * 1024
        ),
    )(embedded, norm_gain.astype(F32), shorts, medium_filters[0], out_weight[0])
    return result[None]


def solution(mesh):
    sizes = tuple(mesh.shape[name] for name in ("section", "seq", "mp"))
    in_specs = (
        P(None, "seq"),
        P(None, "mp"),
        P("section", "mp"),
        P("section", None, None, "mp"),
        P("section", None, "mp"),
        P("section", "seq", "mp"),
    )
    out_specs = P("section", None, "seq", "mp")
    return jax.shard_map(
        functools.partial(local, sizes), mesh=mesh, in_specs=in_specs, out_specs=out_specs, check_vma=False
    )
```

```python
import functools

import jax
import jax.numpy as jnp
from jax import lax
from jax.experimental import pallas as pl
from jax.experimental.pallas import tpu as pltpu
from jax.sharding import PartitionSpec as P

MESH = pl.DeviceIdType.MESH
LANES = 128
BF = jnp.bfloat16
F32 = jnp.float32


def relay_kernel(
    sizes,
    emb_ref, gain_ref, short_ref, med_ref, w_ref,
    out_ref,
    wbuf, inbuf, x, gainf, shortf, colb, sqbuf, nsend, nrim, nf, qf, ext, psend, prim, sh, medf, gbuf, acc,
    own_sem, w_send, w_recv, go_sem, in_send, in_recv, sq_send, sq_recv,
    n_send, n_recv, p_send, p_recv, up_send, up_recv, dn_send, dn_recv,
):
    n_sec, n_seq, n_mp = sizes
    micro, rows, width = emb_ref.shape
    total_width = width * n_mp
    short_len = short_ref.shape[2]
    med_len = med_ref.shape[1]
    rim = psend.shape[1]
    nrim_rows = nsend.shape[1]
    blocks = rows // rim
    depth = w_ref.shape[1]
    half = depth // 2
    levels = n_seq.bit_length() - 1
    sec, seq, mp = lax.axis_index("section"), lax.axis_index("seq"), lax.axis_index("mp")

    def remote(src, dst, send, recv, **where):
        return pltpu.make_async_remote_copy(
            src_ref=src, dst_ref=dst, send_sem=send, recv_sem=recv,
            device_id=where, device_id_type=MESH,
        )

    own = pltpu.make_async_copy(
        w_ref.at[0], wbuf.at[pl.ds(pl.multiple_of(seq * depth, depth), depth)], own_sem
    )
    own.start()
    barrier = pltpu.get_barrier_semaphore()
    greeted = 0
    for axis, count, index in (("section", n_sec, sec), ("seq", n_seq, seq), ("mp", n_mp, mp)):
        for step in range(1, count):
            pl.semaphore_signal(
                barrier, inc=1, device_id={axis: lax.rem(index + step, count)}, device_id_type=MESH
            )
            greeted += 1
    pl.semaphore_wait(barrier, greeted)
    own.wait()

    def bit_of(bit):
        return lax.rem(lax.div(seq, jnp.int32(1 << bit)), jnp.int32(2))

    orders = (list(range(levels)), list(reversed(range(levels))))

    def weight_copies(level, incoming=False):
        made = []
        for part in range(2):
            order = orders[part]
            flip = order[level]
            partner = seq + (1 - 2 * bit_of(flip)) * (1 << flip)
            for k in range(1 << level):
                shard = seq
                theirs = partner
                for i in range(level):
                    change = (((k >> i) & 1) - bit_of(order[i])) * (1 << order[i])
                    shard = shard + change
                    theirs = theirs + change
                slot = (1 << level) - 1 + k
                start = pl.multiple_of((theirs if incoming else shard) * depth + part * half, half)
                place = wbuf.at[pl.ds(start, half)]
                made.append(remote(place, place, w_send.at[part, slot], w_recv.at[part, slot], seq=partner))
        return made

    def weights_start(level):
        for out in weight_copies(level):
            out.start()

    def weights_arrive(level):
        for into in weight_copies(level, True):
            into.wait_recv()

    def weights_forward():
        for level in range(1, levels):
            weights_arrive(level - 1)
            weights_start(level)

    @pl.when(sec > 0)
    def _():
        pl.semaphore_wait(go_sem, 1)

    weights_start(0)

    @pl.when(sec > 0)
    def _():
        weights_forward()

    medf[...] = med_ref[0].astype(F32)
    shortf[...] = short_ref[0].astype(F32)
    gainf[...] = gain_ref[...].astype(F32)

    @pl.when(seq == 0)
    def _():
        nf[0:nrim_rows, :] = jnp.zeros((nrim_rows, width), F32)
        ext[0:rim, :] = jnp.zeros((rim, width), F32)

    def lane(c):
        return pl.ds(pl.multiple_of(c * LANES, LANES), LANES)

    chunks = width // LANES

    def relay_copy(m):
        return remote(out_ref.at[m], inbuf.at[m], in_send.at[m], in_recv.at[m], section=sec + 1)

    def relay_in(m):
        return remote(inbuf.at[m], inbuf.at[m], in_send.at[m], in_recv.at[m], section=sec)

    def square_copy(m, step):
        return remote(
            sqbuf.at[m, mp], sqbuf.at[m, mp], sq_send.at[m, step - 1], sq_recv.at[m, step - 1],
            mp=lax.rem(mp + step, n_mp),
        )

    def square_in(m, step):
        place = sqbuf.at[m, lax.rem(mp + n_mp - step, n_mp)]
        return remote(
            place, place, sq_send.at[m, step - 1], sq_recv.at[m, step - 1],
            mp=lax.rem(mp + step, n_mp),
        )

    def normed_copy(m):
        return remote(nsend.at[m], nrim.at[m], n_send.at[m], n_recv.at[m], seq=seq + 1)

    def product_copy(m):
        return remote(psend.at[m], prim.at[m], p_send.at[m], p_recv.at[m], seq=seq + 1)

    def line_copy(m, block, step, piece, up):
        place = gbuf.at[m, block, pl.ds(piece * rim, rim)]
        send, recv = (up_send, up_recv) if up else (dn_send, dn_recv)
        return remote(
            place, place, send.at[m, step, piece], recv.at[m, step, piece],
            mp=(mp + 1) if up else (mp - 1),
        )

    def gated_send(m, block, step, piece, up):
        room = (mp < n_mp - 1) if up else (mp > 0)

        @pl.when(room)
        def _():
            line_copy(m, block, step, piece, up).start()

    row_chunk = 32

    def forward(m, step):
        for up in (True, False):
            here = (mp - step) if up else (mp + step)
            exists = (here >= 0) if up else (here < n_mp)

            @pl.when(exists)
            def _():
                for piece in reversed(range(blocks)):
                    line_copy(m, here, step - 1, piece, up).wait_recv()
                    if step < n_mp - 1:
                        gated_send(m, here, step, piece, up)

    def front(m):
        pending = list(range(1, n_mp - 1)) if m > 0 else []

        def forward_one():
            if pending:
                forward(m - 1, pending.pop(0))

        @pl.when(sec > 0)
        def _():
            relay_in(m).wait_recv()

        def squares(i, _):
            part = pl.ds(pl.multiple_of(i * row_chunk, row_chunk), row_chunk)

            @pl.when(sec == 0)
            def _():
                x[m, part, :] = emb_ref[m, part, :].astype(F32)

            @pl.when(sec > 0)
            def _():
                x[m, part, :] = inbuf[m, part, :].astype(F32)

            value = x[m, part, :]
            summed = jnp.sum(value * value, axis=1, keepdims=True)
            colb[part, :] = jnp.broadcast_to(summed, (row_chunk, LANES))
            return 0

        lax.fori_loop(0, rows // row_chunk, squares, 0)
        sqbuf[m, mp] = colb[...].T[0:8]
        for step in range(1, n_mp):
            square_copy(m, step).start()
        for step in range(1, n_mp):
            square_in(m, step).wait_recv()
        total = sqbuf[m, 0]
        for j in range(1, n_mp):
            total = total + sqbuf[m, j]
        scale = lax.rsqrt(total / total_width + 1e-06)
        colb[...] = jnp.broadcast_to(scale[0:1], (LANES, rows)).T

        def normalise(c, _):
            value = x[m, :, lane(c)] * colb[...] * gainf[0:1, lane(c)]
            rounded = value.astype(BF)
            nf[pl.ds(nrim_rows, rows), lane(c)] = rounded.astype(F32)
            nsend[m, :, lane(c)] = rounded[rows - nrim_rows:]
            return 0

        lax.fori_loop(0, chunks, normalise, 0)

        @pl.when(seq < n_seq - 1)
        def _():
            normed_copy(m).start()

        forward_one()

        def features(block):
            sub = rim // 2

            def body(c, _):
                for piece in range(2):
                    base = block * rim + piece * sub
                    made = [None, None, None]
                    for s in range(short_len):
                        window = nf[pl.ds(nrim_rows + base - s, sub), lane(c)]
                        for f in range(3):
                            term = shortf[f, pl.ds(s, 1), lane(c)] * window
                            made[f] = term if made[f] is None else made[f] + term
                    made = [value.astype(BF).astype(F32) for value in made]
                    product = (made[1] * made[2]).astype(BF)
                    qf[pl.ds(base, sub), lane(c)] = made[0]
                    ext[pl.ds(rim + base, sub), lane(c)] = product.astype(F32)
                    if block == blocks - 1:
                        psend[m, pl.ds(piece * sub, sub), lane(c)] = product
                return 0

            lax.fori_loop(0, chunks, body, 0)

        for block in reversed(range(blocks)):
            if block == 0:
                @pl.when(seq > 0)
                def _():
                    normed_copy(m).wait_recv()
                    nf[0:nrim_rows, :] = nrim[m].astype(F32)

            features(block)
            if block == blocks - 1:
                @pl.when(seq < n_seq - 1)
                def _():
                    product_copy(m).start()

        forward_one()
        if m == 0:
            @pl.when(sec == 0)
            def _():
                weights_forward()

        def filtering(block):
            taps_rows = 2 * rim

            def body(c, _):
                lo = block * rim
                for b in range(8):
                    sh[b, 8:taps_rows, :] = ext[pl.ds(lo + 8 - b, taps_rows - 8), lane(c)]
                value = jnp.zeros((rim, LANES), F32)
                for b in range(8):
                    for a in range(rim // 8):
                        s = 8 * a + b
                        if s < med_len:
                            tap = medf[pl.ds(s, 1), lane(c)]
                            value = value + tap * sh[b, rim - 8 * a:2 * rim - 8 * a, :]
                here = pl.ds(lo, rim)
                gbuf[m, mp, here, lane(c)] = (qf[here, lane(c)] * value).astype(BF)
                return 0

            lax.fori_loop(0, chunks, body, 0)

        for block in reversed(range(blocks)):
            if block == 0:
                @pl.when(seq > 0)
                def _():
                    product_copy(m).wait_recv()
                    ext[0:rim, :] = prim[m].astype(F32)

            filtering(block)
            for up in (True, False):
                gated_send(m, mp, 0, block, up)

        while pending:
            forward_one()

    cols = 256

    def add_block(m, block, first):
        source = pl.ds(pl.multiple_of(block * width, width), width)

        def body(c, _):
            part = pl.ds(pl.multiple_of(c * cols, cols), cols)
            value = jnp.dot(gbuf[m, block], wbuf[source, part], preferred_element_type=F32)
            if first:
                acc[:, part] = value
            else:
                acc[:, part] += value
            return 0

        lax.fori_loop(0, width // cols, body, 0)

    def back(m):
        if m == 0:
            weights_arrive(levels - 1)

            @pl.when(sec < n_sec - 1)
            def _():
                pl.semaphore_signal(go_sem, inc=1, device_id={"section": sec + 1}, device_id_type=MESH)

        add_block(m, mp, True)
        for step in range(1, n_mp):
            if m == micro - 1 or step == n_mp - 1:
                forward(m, step)
            for up in (True, False):
                here = (mp - step) if up else (mp + step)
                exists = (here >= 0) if up else (here < n_mp)

                @pl.when(exists)
                def _():
                    add_block(m, here, False)

        def finish(i, _):
            part = pl.ds(pl.multiple_of(i * row_chunk, row_chunk), row_chunk)
            out_ref[m, part, :] = (x[m, part, :] + acc[part, :]).astype(BF)
            return 0

        lax.fori_loop(0, rows // row_chunk, finish, 0)

        @pl.when(sec < n_sec - 1)
        def _():
            relay_copy(m).start()

    for m in range(micro + 1):
        if m < micro:
            front(m)
        if m > 0:
            back(m - 1)

    for level in range(levels):
        for out in weight_copies(level):
            out.wait_send()
    for m in range(micro):
        @pl.when(sec < n_sec - 1)
        def _():
            relay_copy(m).wait_send()

        for step in range(1, n_mp):
            square_copy(m, step).wait_send()

        @pl.when(seq < n_seq - 1)
        def _():
            normed_copy(m).wait_send()
            product_copy(m).wait_send()

        for up in (True, False):
            room = (mp < n_mp - 1) if up else (mp > 0)
            for step in range(n_mp - 1):
                block = (mp - step) if up else (mp + step)
                exists = (block >= 0) if up else (block < n_mp)

                @pl.when(jnp.logical_and(room, exists))
                def _():
                    for piece in range(blocks):
                        line_copy(m, block, step, piece, up).wait_send()


def up16(count):
    return (count + 15) // 16 * 16


def local(sizes, token_ids, embed_table, norm_gain, short_filters, medium_filters, out_weight):
    n_sec, n_seq, n_mp = sizes
    micro, rows = token_ids.shape
    vocab, width = embed_table.shape
    ids = token_ids.reshape(micro * rows)
    one_hot = (ids[:, None] == lax.broadcasted_iota(jnp.int32, (micro * rows, vocab), 1)).astype(BF)
    embedded = jnp.dot(one_hot, embed_table, preferred_element_type=F32).astype(BF)
    embedded = embedded.reshape(micro, rows, width)
    nrim_rows = up16(short_filters.shape[2] - 1)
    rim = up16(medium_filters.shape[1])
    blocks = rows // rim
    vmem = pl.BlockSpec(memory_space=pltpu.VMEM)
    dma = pltpu.SemaphoreType.DMA
    result = pl.pallas_call(
        functools.partial(relay_kernel, sizes),
        out_shape=jax.ShapeDtypeStruct((micro, rows, width), BF),
        in_specs=[vmem, vmem, vmem, vmem, pl.BlockSpec(memory_space=pl.ANY)],
        out_specs=vmem,
        scratch_shapes=[
            pltpu.VMEM((width * n_mp, width), BF),
            pltpu.VMEM((micro, rows, width), BF),
            pltpu.VMEM((micro, rows, width), F32),
            pltpu.VMEM(norm_gain.shape, F32),
            pltpu.VMEM(short_filters.shape[1:], F32),
            pltpu.VMEM((rows, LANES), F32),
            pltpu.VMEM((micro, n_mp, 8, rows), F32),
            pltpu.VMEM((micro, nrim_rows, width), BF),
            pltpu.VMEM((micro, nrim_rows, width), BF),
            pltpu.VMEM((nrim_rows + rows, width), F32),
            pltpu.VMEM((rows, width), F32),
            pltpu.VMEM((rim + rows, width), F32),
            pltpu.VMEM((micro, rim, width), BF),
            pltpu.VMEM((micro, rim, width), BF),
            pltpu.VMEM((8, 2 * rim, LANES), F32),
            pltpu.VMEM(medium_filters.shape[1:], F32),
            pltpu.VMEM((micro, n_mp, rows, width), BF),
            pltpu.VMEM((rows, width), F32),
            dma, dma((2, n_seq)), dma((2, n_seq)), pltpu.SemaphoreType.REGULAR,
            dma((micro,)), dma((micro,)), dma((micro, n_mp)), dma((micro, n_mp)),
            dma((micro,)), dma((micro,)), dma((micro,)), dma((micro,)),
            dma((micro, n_mp, blocks)), dma((micro, n_mp, blocks)),
            dma((micro, n_mp, blocks)), dma((micro, n_mp, blocks)),
        ],
        compiler_params=pltpu.CompilerParams(
            collective_id=0, has_side_effects=True, vmem_limit_bytes=56 * 1024 * 1024
        ),
    )(embedded, norm_gain, short_filters, medium_filters, out_weight)
    return result[None]


def solution(mesh):
    sizes = tuple(mesh.shape[name] for name in ("section", "seq", "mp"))
    in_specs = (
        P(None, "seq"),
        P(None, "mp"),
        P("section", "mp"),
        P("section", None, None, "mp"),
        P("section", None, "mp"),
        P("section", "seq", "mp"),
    )
    out_specs = P("section", None, "seq", "mp")
    return jax.shard_map(
        functools.partial(local, sizes), mesh=mesh, in_specs=in_specs, out_specs=out_specs, check_vma=False
    )
```

```python
import functools

import jax
import jax.numpy as jnp
from jax import lax
from jax.experimental import pallas as pl
from jax.experimental.pallas import tpu as pltpu
from jax.sharding import PartitionSpec as P

MESH = pl.DeviceIdType.MESH
LANES = 128
BF = jnp.bfloat16
F32 = jnp.float32


def relay_kernel(
    sizes,
    emb_ref, gain_ref, short_ref, med_ref, w_ref,
    out_ref,
    wbuf, inbuf, x, gainf, shortf, colb, sqbuf, nsend, nrim, nf, qf, ext, psend, prim, sh, medf, gbuf, acc,
    own_sem, w_send, w_recv, go_sem, in_send, in_recv, sq_send, sq_recv,
    n_send, n_recv, p_send, p_recv, up_send, up_recv, dn_send, dn_recv,
):
    n_sec, n_seq, n_mp = sizes
    micro, rows, width = emb_ref.shape
    total_width = width * n_mp
    short_len = short_ref.shape[2]
    med_len = med_ref.shape[1]
    rim = psend.shape[1]
    nrim_rows = nsend.shape[1]
    blocks = rows // rim
    depth = w_ref.shape[1]
    half = depth // 2
    levels = n_seq.bit_length() - 1
    sec, seq, mp = lax.axis_index("section"), lax.axis_index("seq"), lax.axis_index("mp")

    def remote(src, dst, send, recv, **where):
        return pltpu.make_async_remote_copy(
            src_ref=src, dst_ref=dst, send_sem=send, recv_sem=recv,
            device_id=where, device_id_type=MESH,
        )

    own = pltpu.make_async_copy(
        w_ref.at[0], wbuf.at[pl.ds(pl.multiple_of(seq * depth, depth), depth)], own_sem
    )
    own.start()
    barrier = pltpu.get_barrier_semaphore()
    greeted = 0
    for axis, count, index in (("section", n_sec, sec), ("seq", n_seq, seq), ("mp", n_mp, mp)):
        for step in range(1, count):
            pl.semaphore_signal(
                barrier, inc=1, device_id={axis: lax.rem(index + step, count)}, device_id_type=MESH
            )
            greeted += 1
    pl.semaphore_wait(barrier, greeted)
    own.wait()

    def bit_of(bit):
        return lax.rem(lax.div(seq, jnp.int32(1 << bit)), jnp.int32(2))

    orders = (list(range(levels)), list(reversed(range(levels))))

    def weight_copies(level, pieces, incoming=False):
        made = []
        for part in range(2):
            order = orders[part]
            flip = order[level]
            partner = seq + (1 - 2 * bit_of(flip)) * (1 << flip)
            for k in pieces:
                shard = seq
                theirs = partner
                for i in range(level):
                    change = ((k >> i) & 1) * (1 - 2 * bit_of(order[i])) * (1 << order[i])
                    shard = shard + change
                    theirs = theirs + change
                slot = (1 << level) - 1 + k
                start = pl.multiple_of((theirs if incoming else shard) * depth + part * half, half)
                place = wbuf.at[pl.ds(start, half)]
                made.append(remote(place, place, w_send.at[part, slot], w_recv.at[part, slot], seq=partner))
        return made

    def weights_start(stage):
        pieces = range(1) if stage == 0 else range(1 << (stage - 1), 1 << stage)
        for level in range(stage, levels):
            for out in weight_copies(level, pieces):
                out.start()

    def weights_arrive(level):
        for into in weight_copies(level, range(1 << level), True):
            into.wait_recv()

    def weights_forward():
        for stage in range(1, levels):
            weights_arrive(stage - 1)
            weights_start(stage)

    @pl.when(sec > 0)
    def _():
        pl.semaphore_wait(go_sem, 1)

    weights_start(0)

    @pl.when(sec > 0)
    def _():
        weights_forward()

    medf[...] = med_ref[0].astype(F32)
    shortf[...] = short_ref[0].astype(F32)
    gainf[...] = gain_ref[...].astype(F32)

    @pl.when(seq == 0)
    def _():
        nf[0:nrim_rows, :] = jnp.zeros((nrim_rows, width), F32)
        ext[0:rim, :] = jnp.zeros((rim, width), F32)

    def lane(c):
        return pl.ds(pl.multiple_of(c * LANES, LANES), LANES)

    chunks = width // LANES

    def relay_copy(m):
        return remote(out_ref.at[m], inbuf.at[m], in_send.at[m], in_recv.at[m], section=sec + 1)

    def relay_in(m):
        return remote(inbuf.at[m], inbuf.at[m], in_send.at[m], in_recv.at[m], section=sec)

    def square_copy(m, step):
        return remote(
            sqbuf.at[m, mp], sqbuf.at[m, mp], sq_send.at[m, step - 1], sq_recv.at[m, step - 1],
            mp=lax.rem(mp + step, n_mp),
        )

    def square_in(m, step):
        place = sqbuf.at[m, lax.rem(mp + n_mp - step, n_mp)]
        return remote(
            place, place, sq_send.at[m, step - 1], sq_recv.at[m, step - 1],
            mp=lax.rem(mp + step, n_mp),
        )

    def normed_copy(m):
        return remote(nsend.at[m], nrim.at[m], n_send.at[m], n_recv.at[m], seq=seq + 1)

    def product_copy(m):
        return remote(psend.at[m], prim.at[m], p_send.at[m], p_recv.at[m], seq=seq + 1)

    def line_copy(m, block, step, piece, up):
        place = gbuf.at[m, block, pl.ds(piece * rim, rim)]
        send, recv = (up_send, up_recv) if up else (dn_send, dn_recv)
        return remote(
            place, place, send.at[m, step, piece], recv.at[m, step, piece],
            mp=(mp + 1) if up else (mp - 1),
        )

    def gated_send(m, block, step, piece, up):
        room = (mp < n_mp - 1) if up else (mp > 0)

        @pl.when(room)
        def _():
            line_copy(m, block, step, piece, up).start()

    row_chunk = 32

    def own_squares(m, source):
        def body(i, _):
            part = pl.ds(pl.multiple_of(i * row_chunk, row_chunk), row_chunk)
            value = source[m, part, :].astype(F32)
            x[m, part, :] = value
            summed = jnp.sum(value * value, axis=1, keepdims=True)
            colb[part, :] = jnp.broadcast_to(summed, (row_chunk, LANES))
            return 0

        lax.fori_loop(0, rows // row_chunk, body, 0)
        sqbuf[m, mp] = colb[...].T[0:8]

    def send_squares(m):
        for step in range(1, n_mp):
            square_copy(m, step).start()

    @pl.when(sec == 0)
    def _():
        for m in range(micro):
            own_squares(m, emb_ref)
            send_squares(m)

    def forward(m, step):
        for up in (True, False):
            here = (mp - step) if up else (mp + step)
            exists = (here >= 0) if up else (here < n_mp)

            @pl.when(exists)
            def _():
                for piece in reversed(range(blocks)):
                    line_copy(m, here, step - 1, piece, up).wait_recv()
                    if step < n_mp - 1:
                        gated_send(m, here, step, piece, up)

    def weights_done():
        weights_arrive(levels - 1)

        @pl.when(sec < n_sec - 1)
        def _():
            pl.semaphore_signal(go_sem, inc=1, device_id={"section": sec + 1}, device_id_type=MESH)

    def front(m):
        pending = list(range(1, n_mp - 1)) if m > 0 else []

        def forward_one():
            if pending:
                forward(m - 1, pending.pop(0))

        @pl.when(sec > 0)
        def _():
            relay_in(m).wait_recv()
            own_squares(m, inbuf)
            send_squares(m)

        for step in range(1, n_mp):
            square_in(m, step).wait_recv()
        total = sqbuf[m, 0]
        for j in range(1, n_mp):
            total = total + sqbuf[m, j]
        scale = lax.rsqrt(total / total_width + 1e-06)
        colb[...] = jnp.broadcast_to(scale[0:1], (LANES, rows)).T

        def normalise(c, _):
            value = x[m, :, lane(c)] * colb[...] * gainf[0:1, lane(c)]
            rounded = value.astype(BF)
            nf[pl.ds(nrim_rows, rows), lane(c)] = rounded.astype(F32)
            nsend[m, :, lane(c)] = rounded[rows - nrim_rows:]
            return 0

        lax.fori_loop(0, chunks, normalise, 0)

        @pl.when(seq < n_seq - 1)
        def _():
            normed_copy(m).start()

        forward_one()

        def features(block):
            sub = rim // 2

            def body(c, _):
                for piece in range(2):
                    base = block * rim + piece * sub
                    made = [None, None, None]
                    for s in range(short_len):
                        window = nf[pl.ds(nrim_rows + base - s, sub), lane(c)]
                        for f in range(3):
                            term = shortf[f, pl.ds(s, 1), lane(c)] * window
                            made[f] = term if made[f] is None else made[f] + term
                    made = [value.astype(BF).astype(F32) for value in made]
                    product = (made[1] * made[2]).astype(BF)
                    qf[pl.ds(base, sub), lane(c)] = made[0]
                    ext[pl.ds(rim + base, sub), lane(c)] = product.astype(F32)
                    if block == blocks - 1:
                        psend[m, pl.ds(piece * sub, sub), lane(c)] = product
                return 0

            lax.fori_loop(0, chunks, body, 0)

        for block in reversed(range(blocks)):
            if block == 0:
                @pl.when(seq > 0)
                def _():
                    normed_copy(m).wait_recv()
                    nf[0:nrim_rows, :] = nrim[m].astype(F32)

            features(block)
            if block == blocks - 1:
                @pl.when(seq < n_seq - 1)
                def _():
                    product_copy(m).start()

        forward_one()
        if m == 0:
            @pl.when(sec == 0)
            def _():
                weights_forward()
        if m == min(1, micro - 1):
            @pl.when(sec == 0)
            def _():
                weights_done()

        def filtering(block):
            taps_rows = 2 * rim

            def body(c, _):
                lo = block * rim
                for b in range(8):
                    sh[b, 8:taps_rows, :] = ext[pl.ds(lo + 8 - b, taps_rows - 8), lane(c)]
                value = jnp.zeros((rim, LANES), F32)
                for b in range(8):
                    for a in range(rim // 8):
                        s = 8 * a + b
                        if s < med_len:
                            tap = medf[pl.ds(s, 1), lane(c)]
                            value = value + tap * sh[b, rim - 8 * a:2 * rim - 8 * a, :]
                here = pl.ds(lo, rim)
                gbuf[m, mp, here, lane(c)] = (qf[here, lane(c)] * value).astype(BF)
                return 0

            lax.fori_loop(0, chunks, body, 0)

        for block in reversed(range(blocks)):
            if block == 0:
                @pl.when(seq > 0)
                def _():
                    product_copy(m).wait_recv()
                    ext[0:rim, :] = prim[m].astype(F32)

            filtering(block)
            for up in (True, False):
                gated_send(m, mp, 0, block, up)

        while pending:
            forward_one()

    cols = 256

    def add_block(m, block, first):
        source = pl.ds(pl.multiple_of(block * width, width), width)

        def body(c, _):
            part = pl.ds(pl.multiple_of(c * cols, cols), cols)
            value = jnp.dot(gbuf[m, block], wbuf[source, part], preferred_element_type=F32)
            if first:
                acc[:, part] = value
            else:
                acc[:, part] += value
            return 0

        lax.fori_loop(0, width // cols, body, 0)

    def back(m):
        if m == 0:
            @pl.when(sec > 0)
            def _():
                weights_done()

        add_block(m, mp, True)
        for step in range(1, n_mp):
            if m == micro - 1 or step == n_mp - 1:
                forward(m, step)
            for up in (True, False):
                here = (mp - step) if up else (mp + step)
                exists = (here >= 0) if up else (here < n_mp)

                @pl.when(exists)
                def _():
                    add_block(m, here, False)

        def finish(i, _):
            part = pl.ds(pl.multiple_of(i * row_chunk, row_chunk), row_chunk)
            out_ref[m, part, :] = (x[m, part, :] + acc[part, :]).astype(BF)
            return 0

        lax.fori_loop(0, rows // row_chunk, finish, 0)

        @pl.when(sec < n_sec - 1)
        def _():
            relay_copy(m).start()

    for m in range(micro + 1):
        if m < micro:
            front(m)
        if m > 0:
            back(m - 1)

    for level in range(levels):
        for out in weight_copies(level, range(1 << level)):
            out.wait_send()
    for m in range(micro):
        @pl.when(sec < n_sec - 1)
        def _():
            relay_copy(m).wait_send()

        for step in range(1, n_mp):
            square_copy(m, step).wait_send()

        @pl.when(seq < n_seq - 1)
        def _():
            normed_copy(m).wait_send()
            product_copy(m).wait_send()

        for up in (True, False):
            room = (mp < n_mp - 1) if up else (mp > 0)
            for step in range(n_mp - 1):
                block = (mp - step) if up else (mp + step)
                exists = (block >= 0) if up else (block < n_mp)

                @pl.when(jnp.logical_and(room, exists))
                def _():
                    for piece in range(blocks):
                        line_copy(m, block, step, piece, up).wait_send()


def up16(count):
    return (count + 15) // 16 * 16


def local(sizes, token_ids, embed_table, norm_gain, short_filters, medium_filters, out_weight):
    n_sec, n_seq, n_mp = sizes
    micro, rows = token_ids.shape
    vocab, width = embed_table.shape
    ids = token_ids.reshape(micro * rows)
    one_hot = (ids[:, None] == lax.broadcasted_iota(jnp.int32, (micro * rows, vocab), 1)).astype(BF)
    embedded = jnp.dot(one_hot, embed_table, preferred_element_type=F32).astype(BF)
    embedded = embedded.reshape(micro, rows, width)
    nrim_rows = up16(short_filters.shape[2] - 1)
    rim = up16(medium_filters.shape[1])
    blocks = rows // rim
    vmem = pl.BlockSpec(memory_space=pltpu.VMEM)
    dma = pltpu.SemaphoreType.DMA
    result = pl.pallas_call(
        functools.partial(relay_kernel, sizes),
        out_shape=jax.ShapeDtypeStruct((micro, rows, width), BF),
        in_specs=[vmem, vmem, vmem, vmem, pl.BlockSpec(memory_space=pl.ANY)],
        out_specs=vmem,
        scratch_shapes=[
            pltpu.VMEM((width * n_mp, width), BF),
            pltpu.VMEM((micro, rows, width), BF),
            pltpu.VMEM((micro, rows, width), F32),
            pltpu.VMEM(norm_gain.shape, F32),
            pltpu.VMEM(short_filters.shape[1:], F32),
            pltpu.VMEM((rows, LANES), F32),
            pltpu.VMEM((micro, n_mp, 8, rows), F32),
            pltpu.VMEM((micro, nrim_rows, width), BF),
            pltpu.VMEM((micro, nrim_rows, width), BF),
            pltpu.VMEM((nrim_rows + rows, width), F32),
            pltpu.VMEM((rows, width), F32),
            pltpu.VMEM((rim + rows, width), F32),
            pltpu.VMEM((micro, rim, width), BF),
            pltpu.VMEM((micro, rim, width), BF),
            pltpu.VMEM((8, 2 * rim, LANES), F32),
            pltpu.VMEM(medium_filters.shape[1:], F32),
            pltpu.VMEM((micro, n_mp, rows, width), BF),
            pltpu.VMEM((rows, width), F32),
            dma, dma((2, n_seq)), dma((2, n_seq)), pltpu.SemaphoreType.REGULAR,
            dma((micro,)), dma((micro,)), dma((micro, n_mp)), dma((micro, n_mp)),
            dma((micro,)), dma((micro,)), dma((micro,)), dma((micro,)),
            dma((micro, n_mp, blocks)), dma((micro, n_mp, blocks)),
            dma((micro, n_mp, blocks)), dma((micro, n_mp, blocks)),
        ],
        compiler_params=pltpu.CompilerParams(
            collective_id=0, has_side_effects=True, vmem_limit_bytes=56 * 1024 * 1024
        ),
    )(embedded, norm_gain, short_filters, medium_filters, out_weight)
    return result[None]


def solution(mesh):
    sizes = tuple(mesh.shape[name] for name in ("section", "seq", "mp"))
    in_specs = (
        P(None, "seq"),
        P(None, "mp"),
        P("section", "mp"),
        P("section", None, None, "mp"),
        P("section", None, "mp"),
        P("section", "seq", "mp"),
    )
    out_specs = P("section", None, "seq", "mp")
    return jax.shard_map(
        functools.partial(local, sizes), mesh=mesh, in_specs=in_specs, out_specs=out_specs, check_vma=False
    )
```

```python
import functools

import jax
import jax.numpy as jnp
from jax import lax
from jax.experimental import pallas as pl
from jax.experimental.pallas import tpu as pltpu
from jax.sharding import PartitionSpec as P

MESH = pl.DeviceIdType.MESH
LANES = 128
BF = jnp.bfloat16
F32 = jnp.float32


def relay_kernel(
    sizes,
    emb_ref, gain_ref, short_ref, med_ref, w_ref,
    out_ref,
    wbuf, inbuf, x, gainf, shortf, colb, sqbuf, nsend, nrim, nf, qf, ext, psend, prim, sh, medf, gbuf, acc,
    own_sem, w_send, w_recv, go_sem, in_send, in_recv, sq_send, sq_recv,
    n_send, n_recv, p_send, p_recv, up_send, up_recv, dn_send, dn_recv,
):
    n_sec, n_seq, n_mp = sizes
    micro, rows, width = emb_ref.shape
    total_width = width * n_mp
    short_len = short_ref.shape[2]
    med_len = med_ref.shape[1]
    rim = psend.shape[1]
    nrim_rows = nsend.shape[1]
    blocks = rows // rim
    depth = w_ref.shape[1]
    half = depth // 2
    levels = n_seq.bit_length() - 1
    sec, seq, mp = lax.axis_index("section"), lax.axis_index("seq"), lax.axis_index("mp")

    def remote(src, dst, send, recv, **where):
        return pltpu.make_async_remote_copy(
            src_ref=src, dst_ref=dst, send_sem=send, recv_sem=recv,
            device_id=where, device_id_type=MESH,
        )

    own = pltpu.make_async_copy(
        w_ref.at[0], wbuf.at[pl.ds(pl.multiple_of(seq * depth, depth), depth)], own_sem
    )
    own.start()
    barrier = pltpu.get_barrier_semaphore()
    greeted = 0
    for axis, count, index in (("section", n_sec, sec), ("seq", n_seq, seq), ("mp", n_mp, mp)):
        for step in range(1, count):
            pl.semaphore_signal(
                barrier, inc=1, device_id={axis: lax.rem(index + step, count)}, device_id_type=MESH
            )
            greeted += 1
    pl.semaphore_wait(barrier, greeted)
    own.wait()

    def bit_of(bit):
        return lax.rem(lax.div(seq, jnp.int32(1 << bit)), jnp.int32(2))

    orders = (list(range(levels)), list(reversed(range(levels))))

    def weight_copies(level, pieces, incoming=False):
        made = []
        for part in range(2):
            order = orders[part]
            flip = order[level]
            partner = seq + (1 - 2 * bit_of(flip)) * (1 << flip)
            for k in pieces:
                shard = seq
                theirs = partner
                for i in range(level):
                    change = ((k >> i) & 1) * (1 - 2 * bit_of(order[i])) * (1 << order[i])
                    shard = shard + change
                    theirs = theirs + change
                slot = (1 << level) - 1 + k
                start = pl.multiple_of((theirs if incoming else shard) * depth + part * half, half)
                place = wbuf.at[pl.ds(start, half)]
                made.append(remote(place, place, w_send.at[part, slot], w_recv.at[part, slot], seq=partner))
        return made

    def weights_start(stage):
        for level in (stage,):
            for out in weight_copies(level, range(1 << stage)):
                out.start()

    def weights_arrive(level):
        for into in weight_copies(level, range(1 << level), True):
            into.wait_recv()

    def weights_forward():
        for stage in range(1, levels):
            weights_arrive(stage - 1)
            weights_start(stage)

    @pl.when(sec > 0)
    def _():
        pl.semaphore_wait(go_sem, 1)

    weights_start(0)

    @pl.when(sec > 0)
    def _():
        weights_forward()

    medf[...] = med_ref[0].astype(F32)
    shortf[...] = short_ref[0].astype(F32)
    gainf[...] = gain_ref[...].astype(F32)

    @pl.when(seq == 0)
    def _():
        nf[0:nrim_rows, :] = jnp.zeros((nrim_rows, width), F32)
        ext[0:rim, :] = jnp.zeros((rim, width), F32)

    def lane(c):
        return pl.ds(pl.multiple_of(c * LANES, LANES), LANES)

    chunks = width // LANES

    def relay_copy(m):
        return remote(out_ref.at[m], inbuf.at[m], in_send.at[m], in_recv.at[m], section=sec + 1)

    def relay_in(m):
        return remote(inbuf.at[m], inbuf.at[m], in_send.at[m], in_recv.at[m], section=sec)

    def square_copy(m, step):
        return remote(
            sqbuf.at[m, mp], sqbuf.at[m, mp], sq_send.at[m, step - 1], sq_recv.at[m, step - 1],
            mp=lax.rem(mp + step, n_mp),
        )

    def square_in(m, step):
        place = sqbuf.at[m, lax.rem(mp + n_mp - step, n_mp)]
        return remote(
            place, place, sq_send.at[m, step - 1], sq_recv.at[m, step - 1],
            mp=lax.rem(mp + step, n_mp),
        )

    def normed_copy(m):
        return remote(nsend.at[m], nrim.at[m], n_send.at[m], n_recv.at[m], seq=seq + 1)

    def product_copy(m):
        return remote(psend.at[m], prim.at[m], p_send.at[m], p_recv.at[m], seq=seq + 1)

    def line_copy(m, block, step, piece, up):
        place = gbuf.at[m, block, pl.ds(piece * rim, rim)]
        send, recv = (up_send, up_recv) if up else (dn_send, dn_recv)
        return remote(
            place, place, send.at[m, step, piece], recv.at[m, step, piece],
            mp=(mp + 1) if up else (mp - 1),
        )

    def gated_send(m, block, step, piece, up):
        room = (mp < n_mp - 1) if up else (mp > 0)

        @pl.when(room)
        def _():
            line_copy(m, block, step, piece, up).start()

    row_chunk = 32

    def own_squares(m, source):
        def body(i, _):
            part = pl.ds(pl.multiple_of(i * row_chunk, row_chunk), row_chunk)
            value = source[m, part, :].astype(F32)
            x[m, part, :] = value
            summed = jnp.sum(value * value, axis=1, keepdims=True)
            colb[part, :] = jnp.broadcast_to(summed, (row_chunk, LANES))
            return 0

        lax.fori_loop(0, rows // row_chunk, body, 0)
        sqbuf[m, mp] = colb[...].T[0:8]

    def send_squares(m):
        for step in range(1, n_mp):
            square_copy(m, step).start()

    @pl.when(sec == 0)
    def _():
        for m in range(micro):
            own_squares(m, emb_ref)
            send_squares(m)

    def forward(m, step):
        for up in (True, False):
            here = (mp - step) if up else (mp + step)
            exists = (here >= 0) if up else (here < n_mp)

            @pl.when(exists)
            def _():
                for piece in reversed(range(blocks)):
                    line_copy(m, here, step - 1, piece, up).wait_recv()
                    if step < n_mp - 1:
                        gated_send(m, here, step, piece, up)

    def weights_done():
        weights_arrive(levels - 1)

    def front(m):
        if m == min(1, micro - 1):
            @pl.when(sec < n_sec - 1)
            def _():
                pl.semaphore_signal(
                    go_sem, inc=1, device_id={"section": sec + 1}, device_id_type=MESH
                )

        pending = list(range(1, n_mp - 1)) if m > 0 else []

        def forward_one():
            if pending:
                forward(m - 1, pending.pop(0))

        @pl.when(sec > 0)
        def _():
            relay_in(m).wait_recv()
            own_squares(m, inbuf)
            send_squares(m)

        for step in range(1, n_mp):
            square_in(m, step).wait_recv()
        total = sqbuf[m, 0]
        for j in range(1, n_mp):
            total = total + sqbuf[m, j]
        scale = lax.rsqrt(total / total_width + 1e-06)
        colb[...] = jnp.broadcast_to(scale[0:1], (LANES, rows)).T

        def normalise(c, _):
            value = x[m, :, lane(c)] * colb[...] * gainf[0:1, lane(c)]
            rounded = value.astype(BF)
            nf[pl.ds(nrim_rows, rows), lane(c)] = rounded.astype(F32)
            nsend[m, :, lane(c)] = rounded[rows - nrim_rows:]
            return 0

        lax.fori_loop(0, chunks, normalise, 0)

        @pl.when(seq < n_seq - 1)
        def _():
            normed_copy(m).start()

        forward_one()

        def features(block):
            sub = rim // 2

            def body(c, _):
                for piece in range(2):
                    base = block * rim + piece * sub
                    made = [None, None, None]
                    for s in range(short_len):
                        window = nf[pl.ds(nrim_rows + base - s, sub), lane(c)]
                        for f in range(3):
                            term = shortf[f, pl.ds(s, 1), lane(c)] * window
                            made[f] = term if made[f] is None else made[f] + term
                    made = [value.astype(BF).astype(F32) for value in made]
                    product = (made[1] * made[2]).astype(BF)
                    qf[pl.ds(base, sub), lane(c)] = made[0]
                    ext[pl.ds(rim + base, sub), lane(c)] = product.astype(F32)
                    if block == blocks - 1:
                        psend[m, pl.ds(piece * sub, sub), lane(c)] = product
                return 0

            lax.fori_loop(0, chunks, body, 0)

        for block in reversed(range(blocks)):
            if block == 0:
                @pl.when(seq > 0)
                def _():
                    normed_copy(m).wait_recv()
                    nf[0:nrim_rows, :] = nrim[m].astype(F32)

            features(block)
            if block == blocks - 1:
                @pl.when(seq < n_seq - 1)
                def _():
                    product_copy(m).start()

        forward_one()
        if m == 0:
            @pl.when(sec == 0)
            def _():
                weights_forward()
        if m == min(1, micro - 1):
            @pl.when(sec == 0)
            def _():
                weights_done()

        def filtering(block):
            taps_rows = 2 * rim

            def body(c, _):
                lo = block * rim
                for b in range(8):
                    sh[b, 8:taps_rows, :] = ext[pl.ds(lo + 8 - b, taps_rows - 8), lane(c)]
                value = jnp.zeros((rim, LANES), F32)
                for b in range(8):
                    for a in range(rim // 8):
                        s = 8 * a + b
                        if s < med_len:
                            tap = medf[pl.ds(s, 1), lane(c)]
                            value = value + tap * sh[b, rim - 8 * a:2 * rim - 8 * a, :]
                here = pl.ds(lo, rim)
                gbuf[m, mp, here, lane(c)] = (qf[here, lane(c)] * value).astype(BF)
                return 0

            lax.fori_loop(0, chunks, body, 0)

        for block in reversed(range(blocks)):
            if block == 0:
                @pl.when(seq > 0)
                def _():
                    product_copy(m).wait_recv()
                    ext[0:rim, :] = prim[m].astype(F32)

            filtering(block)
            for up in (True, False):
                gated_send(m, mp, 0, block, up)

        while pending:
            forward_one()

    cols = 256

    def add_block(m, block, first):
        source = pl.ds(pl.multiple_of(block * width, width), width)

        def body(c, _):
            part = pl.ds(pl.multiple_of(c * cols, cols), cols)
            value = jnp.dot(gbuf[m, block], wbuf[source, part], preferred_element_type=F32)
            if first:
                acc[:, part] = value
            else:
                acc[:, part] += value
            return 0

        lax.fori_loop(0, width // cols, body, 0)

    def back(m):
        if m == 0:
            @pl.when(sec > 0)
            def _():
                weights_done()

        add_block(m, mp, True)
        for step in range(1, n_mp):
            if m == micro - 1 or step == n_mp - 1:
                forward(m, step)
            for up in (True, False):
                here = (mp - step) if up else (mp + step)
                exists = (here >= 0) if up else (here < n_mp)

                @pl.when(exists)
                def _():
                    add_block(m, here, False)

        def finish(i, _):
            part = pl.ds(pl.multiple_of(i * row_chunk, row_chunk), row_chunk)
            out_ref[m, part, :] = (x[m, part, :] + acc[part, :]).astype(BF)
            return 0

        lax.fori_loop(0, rows // row_chunk, finish, 0)

        @pl.when(sec < n_sec - 1)
        def _():
            relay_copy(m).start()

    for m in range(micro + 1):
        if m < micro:
            front(m)
        if m > 0:
            back(m - 1)

    for level in range(levels):
        for out in weight_copies(level, range(1 << level)):
            out.wait_send()
    for m in range(micro):
        @pl.when(sec < n_sec - 1)
        def _():
            relay_copy(m).wait_send()

        for step in range(1, n_mp):
            square_copy(m, step).wait_send()

        @pl.when(seq < n_seq - 1)
        def _():
            normed_copy(m).wait_send()
            product_copy(m).wait_send()

        for up in (True, False):
            room = (mp < n_mp - 1) if up else (mp > 0)
            for step in range(n_mp - 1):
                block = (mp - step) if up else (mp + step)
                exists = (block >= 0) if up else (block < n_mp)

                @pl.when(jnp.logical_and(room, exists))
                def _():
                    for piece in range(blocks):
                        line_copy(m, block, step, piece, up).wait_send()


def up16(count):
    return (count + 15) // 16 * 16


def local(sizes, token_ids, embed_table, norm_gain, short_filters, medium_filters, out_weight):
    n_sec, n_seq, n_mp = sizes
    micro, rows = token_ids.shape
    vocab, width = embed_table.shape
    ids = token_ids.reshape(micro * rows)
    one_hot = (ids[:, None] == lax.broadcasted_iota(jnp.int32, (micro * rows, vocab), 1)).astype(BF)
    embedded = jnp.dot(one_hot, embed_table, preferred_element_type=F32).astype(BF)
    embedded = embedded.reshape(micro, rows, width)
    nrim_rows = up16(short_filters.shape[2] - 1)
    rim = up16(medium_filters.shape[1])
    blocks = rows // rim
    vmem = pl.BlockSpec(memory_space=pltpu.VMEM)
    dma = pltpu.SemaphoreType.DMA
    result = pl.pallas_call(
        functools.partial(relay_kernel, sizes),
        out_shape=jax.ShapeDtypeStruct((micro, rows, width), BF),
        in_specs=[vmem, vmem, vmem, vmem, pl.BlockSpec(memory_space=pl.ANY)],
        out_specs=vmem,
        scratch_shapes=[
            pltpu.VMEM((width * n_mp, width), BF),
            pltpu.VMEM((micro, rows, width), BF),
            pltpu.VMEM((micro, rows, width), F32),
            pltpu.VMEM(norm_gain.shape, F32),
            pltpu.VMEM(short_filters.shape[1:], F32),
            pltpu.VMEM((rows, LANES), F32),
            pltpu.VMEM((micro, n_mp, 8, rows), F32),
            pltpu.VMEM((micro, nrim_rows, width), BF),
            pltpu.VMEM((micro, nrim_rows, width), BF),
            pltpu.VMEM((nrim_rows + rows, width), F32),
            pltpu.VMEM((rows, width), F32),
            pltpu.VMEM((rim + rows, width), F32),
            pltpu.VMEM((micro, rim, width), BF),
            pltpu.VMEM((micro, rim, width), BF),
            pltpu.VMEM((8, 2 * rim, LANES), F32),
            pltpu.VMEM(medium_filters.shape[1:], F32),
            pltpu.VMEM((micro, n_mp, rows, width), BF),
            pltpu.VMEM((rows, width), F32),
            dma, dma((2, n_seq)), dma((2, n_seq)), pltpu.SemaphoreType.REGULAR,
            dma((micro,)), dma((micro,)), dma((micro, n_mp)), dma((micro, n_mp)),
            dma((micro,)), dma((micro,)), dma((micro,)), dma((micro,)),
            dma((micro, n_mp, blocks)), dma((micro, n_mp, blocks)),
            dma((micro, n_mp, blocks)), dma((micro, n_mp, blocks)),
        ],
        compiler_params=pltpu.CompilerParams(
            collective_id=0, has_side_effects=True, vmem_limit_bytes=56 * 1024 * 1024
        ),
    )(embedded, norm_gain, short_filters, medium_filters, out_weight)
    return result[None]


def solution(mesh):
    sizes = tuple(mesh.shape[name] for name in ("section", "seq", "mp"))
    in_specs = (
        P(None, "seq"),
        P(None, "mp"),
        P("section", "mp"),
        P("section", None, None, "mp"),
        P("section", None, "mp"),
        P("section", "seq", "mp"),
    )
    out_specs = P("section", None, "seq", "mp")
    return jax.shard_map(
        functools.partial(local, sizes), mesh=mesh, in_specs=in_specs, out_specs=out_specs, check_vma=False
    )
```
